32 devices in a mesh: rep: 4 (over x, y), pp: 8 (over z, core).
Axes of the slice: x: 2, y: 2, z: 4, core: 2. Of those that a mesh axis runs over, the one named last changes fastest.
Arguments:
- x: bfloat16 [64, 512, 512], P('rep'), parts along dimension 0
- dy: bfloat16 [64, 512, 512], P('rep'), parts along dimension 0
- w_gate: bfloat16 [8, 512, 1408], P('pp')
- w_up: bfloat16 [8, 512, 1408], P('pp')
- w_down: bfloat16 [8, 1408, 512], P('pp')
Outputs:
- output 1: bfloat16 [32, 512, 1408], P(('rep', 'pp')), parts along dimension 0
- output 2: bfloat16 [32, 512, 1408], P(('rep', 'pp')), parts along dimension 0
- output 3: bfloat16 [32, 1408, 512], P(('rep', 'pp')), parts along dimension 0
There are 4 independent parts. The reference program is written for one: setup_inputs(seed, part) draws one part's arguments, and reference() takes and returns one part's arrays. A program takes and returns all parts, laid end to end along the dimension named above; an argument that names none is the same for every part.
All inputs are finite; a program needn't handle non-finite values.
Results may differ from the reference program's by a relative error of at most 0.0262.
Values are sent between devices in bfloat16 or wider.
A program may use at most 2 GiB of HBM per device.

```python
import jax
import jax.numpy as jnp
from jax import lax

MICRO = 16
TOKENS = 512
D = 512
FF = 1408
LAYERS = 8
NAMES = ("w_gate", "w_up", "w_down")
SHAPES = {"w_gate": (LAYERS, D, FF), "w_up": (LAYERS, D, FF), "w_down": (LAYERS, FF, D)}


def bump(key, n, height):
    away = (jnp.arange(n, dtype=jnp.int32) - jax.random.randint(key, (), 0, n, jnp.int32)) % n
    return jnp.where(away < n // 8, height, 1.0)


def together(key, own, strength):
    shared = jax.random.normal(key, own.shape[1:], jnp.float32)
    return (own + strength * shared) * lax.rsqrt(1 + strength * strength)


def setup_inputs(seed: int = 0, part: int = 0) -> dict:
    kx, kdy, ka, kb, kz, kf, kh, kl, *kw = jax.random.split(jax.random.key(seed), 8 + len(NAMES))
    kx, kdy, ka, kb = (jax.random.fold_in(k, part) for k in (kx, kdy, ka, kb))
    shape = (MICRO, TOKENS, D)
    much_x, much_dy = jax.random.uniform(kz, (2,), jnp.float32, 0.0, 1.0)
    layers = 2.0 ** jax.random.uniform(kl, (LAYERS, 1, 1), jnp.float32, -1.0, 1.0)
    x = together(ka, jax.random.normal(kx, shape, jnp.float32), much_x) * bump(kf, D, 4.0)
    dy = together(kb, jax.random.normal(kdy, shape, jnp.float32), much_dy)
    drawn = {"x": x.astype(jnp.bfloat16), "dy": (dy * (MICRO * TOKENS) ** -0.5).astype(jnp.bfloat16)}
    for key, name in zip(kw, NAMES, strict=True):
        w = jax.random.normal(key, SHAPES[name], jnp.float32) * SHAPES[name][1] ** -0.5
        drawn[name] = (w * {"w_gate": 1.0, "w_up": bump(kh, FF, 4.0), "w_down": layers}[name]).astype(jnp.bfloat16)
    return drawn


def matmul(a, w):
    return jnp.dot(a, w, preferred_element_type=jnp.float32).astype(jnp.bfloat16)


def normed(h):
    wide = h.astype(jnp.float32)
    scale = lax.rsqrt(jnp.mean(wide**2, -1, keepdims=True) + 1e-6)
    return (wide * scale).astype(jnp.bfloat16)


def layer(h, w):
    a = normed(h)
    gate = jnp.dot(a, w["w_gate"], preferred_element_type=jnp.float32)
    up = jnp.dot(a, w["w_up"], preferred_element_type=jnp.float32)
    return h + matmul((jax.nn.silu(gate) * up).astype(jnp.bfloat16), w["w_down"])


def stack(weights, h):
    return lax.scan(lambda h, w: (layer(h, w), None), h, weights)[0]


def reference(x, dy, w_gate, w_up, w_down):
    weights = dict(zip(NAMES, (w_gate, w_up, w_down), strict=True))

    def take(so_far, one):
        h, by_y = one
        _, back = jax.vjp(lambda w: stack(w, h), weights)
        return jax.tree.map(lambda total, term: total + term.astype(jnp.float32), so_far, back(by_y)[0]), None

    none_yet = {name: jnp.zeros(w.shape, jnp.float32) for name, w in weights.items()}
    by_weights, _ = lax.scan(take, none_yet, (x, dy))
    return tuple(by_weights[name].astype(jnp.bfloat16) for name in NAMES)
```

```python
import functools

import jax
import jax.numpy as jnp
from jax import lax
from jax.experimental import pallas as pl
from jax.experimental.pallas import tpu as pltpu
from jax.sharding import PartitionSpec as P

F32, BF16 = jnp.float32, jnp.bfloat16
CHUNKS = 2
SLOTS = 4
LAG = 1
WARM = (10, 9, 7, 6, 4, 3, 1, 0)
TILE = 256


def dot(a, b):
    return jnp.dot(a, b, preferred_element_type=F32)


def columns(ff):
    full, rest = divmod(ff, TILE)
    out = [(j * TILE, ff + rest + j * TILE, TILE) for j in range(full)]
    if rest:
        out.append((full * TILE, ff, rest))
    return out


def kernel(cfg, x_ref, dy_ref, wg_ref, wu_ref, wd_ref, og_ref, ou_ref, od_ref, hin, din, wgu, wgut, wd, wdt, acc_gu, acc_d, hout, bout,
           dgu, hid, abuf, at, dyt, hidf, fsem, bsem, fsend, bsend, wsem, osem):
    micro, tokens, d, ff, stages, warms = cfg
    chunks, slots = CHUNKS, SLOTS
    rows = tokens // chunks
    full, rest = divmod(ff, TILE)
    body = full * TILE
    me = lax.axis_index("pp")
    last = stages - 1

    def up_parts():
        parts = [((0, body), (ff + rest, body))]
        if rest:
            parts.append(((body, rest), (ff, rest)))
        return parts

    loads = [pltpu.make_async_copy(wg_ref.at[0], wgu.at[:, pl.ds(0, ff)], wsem.at[0])]
    for n, (src, dst) in enumerate(up_parts()):
        loads.append(pltpu.make_async_copy(wu_ref.at[0, :, pl.ds(*src)], wgu.at[:, pl.ds(*dst)], wsem.at[1 + n]))
    loads.append(pltpu.make_async_copy(wd_ref.at[0], wd, wsem.at[3]))

    def h_in(m, c):
        r = pl.ds(pl.multiple_of(c * rows, rows), rows)
        return pltpu.make_async_copy(x_ref.at[m, r], hin.at[m, r], fsem.at[m, c])

    def d_in(m, c):
        r = pl.ds(pl.multiple_of(c * rows, rows), rows)
        return pltpu.make_async_copy(dy_ref.at[m, r], din.at[m, r], bsem.at[m, c])

    def each(make):
        def go(n, _):
            make(n // chunks, lax.rem(n, chunks)).start()
            return 0

        lax.fori_loop(0, micro * chunks, go, 0)

    @pl.when(me == 0)
    def _():
        h_in(0, 0).start()

    for copy in loads:
        copy.start()

    @pl.when(me == 0)
    def _():
        def go(n, _):
            h_in(n // chunks, lax.rem(n, chunks)).start()
            return 0

        lax.fori_loop(1, micro * chunks, go, 0)

    @pl.when(me == last)
    def _():
        each(d_in)

    barrier = pltpu.get_barrier_semaphore()

    @pl.when(me > 0)
    def _():
        pl.semaphore_signal(barrier, inc=1, device_id={"pp": me - 1})

    @pl.when(me < last)
    def _():
        pl.semaphore_signal(barrier, inc=1, device_id={"pp": me + 1})

    @pl.when((me > 0) & (me < last))
    def _():
        pl.semaphore_wait(barrier, 2)

    @pl.when((me == 0) | (me == last))
    def _():
        pl.semaphore_wait(barrier, 1)

    for copy in loads:
        copy.wait()

    def f_send(m, c):
        r = pl.ds(pl.multiple_of(c * rows, rows), rows)
        s = lax.rem(m, slots)
        return pltpu.make_async_remote_copy(
            src_ref=hout.at[s, r], dst_ref=hin.at[m, r], send_sem=fsend.at[s, c], recv_sem=fsem.at[m, c], device_id={"pp": me + 1})

    def b_send(m, c):
        r = pl.ds(pl.multiple_of(c * rows, rows), rows)
        s = lax.rem(m, slots)
        return pltpu.make_async_remote_copy(
            src_ref=bout.at[s, r], dst_ref=din.at[m, r], send_sem=bsend.at[s, c], recv_sem=bsem.at[m, c], device_id={"pp": me - 1})

    def scale_of(wide):
        return lax.rsqrt(jnp.mean(wide * wide, -1, keepdims=True) + 1e-6)

    def forward(m):
        def piece(c, _):
            r = pl.ds(pl.multiple_of(c * rows, rows), rows)
            h_in(m, c).wait()

            @pl.when(m >= slots)
            def _():
                f_send(m - slots, c).wait_send()

            h = hin[m, r]
            wide = h.astype(F32)
            a = (wide * scale_of(wide)).astype(BF16)
            for g0, u0, w in columns(ff):
                if w == TILE:
                    g, u = dot(a, wgu[:, g0:g0 + w]), dot(a, wgu[:, u0:u0 + w])
                else:
                    gu = dot(a, wgu[:, g0:g0 + 2 * w])
                    g, u = gu[:, :w], gu[:, w:]
                hidf[:, g0:g0 + w] = (g * lax.logistic(g) * u).astype(BF16)
            hout[lax.rem(m, slots), r] = h + dot(hidf[...], wd[...]).astype(BF16)
            f_send(m, c).start()
            return 0

        lax.fori_loop(0, chunks, piece, 0)

    def backward(m):
        s = lax.rem(m, LAG + 1)

        def piece(c, _):
            r = pl.ds(pl.multiple_of(c * rows, rows), rows)

            @pl.when(me == last)
            def _():
                h_in(m, c).wait()

            d_in(m, c).wait()

            h = hin[m, r]
            wide = h.astype(F32)
            a = (wide * scale_of(wide)).astype(BF16)
            abuf[s, r] = a
            by_y = din[m, r]
            for g0, u0, w in columns(ff):
                if w == TILE:
                    g, u = dot(a, wgu[:, g0:g0 + w]), dot(a, wgu[:, u0:u0 + w])
                else:
                    gu = dot(a, wgu[:, g0:g0 + 2 * w])
                    g, u = gu[:, :w], gu[:, w:]
                by_z = dot(by_y, wdt[:, g0:g0 + w]).astype(BF16).astype(F32)
                sig = lax.logistic(g)
                silu = g * sig
                hid[s, r, g0:g0 + w] = (silu * u).astype(BF16)
                dgu[s, r, g0:g0 + w] = (by_z * u * (sig + silu * (1.0 - sig))).astype(BF16)
                dgu[s, r, u0:u0 + w] = (by_z * silu).astype(BF16)

            @pl.when(me > 0)
            def _():
                @pl.when(m >= slots)
                def _():
                    b_send(m - slots, c).wait_send()

                by_a = dot(dgu[s, r, :ff], wgut[:ff]).astype(BF16) + dot(dgu[s, r, ff:], wgut[ff:]).astype(BF16)
                by_a = by_a.astype(F32)
                wide = hin[m, r].astype(F32)
                scale = scale_of(wide)
                by_scale = jnp.sum(by_a * wide, -1, keepdims=True)
                by_wide = by_a * scale - wide * (by_scale * scale * scale * scale * (1.0 / d))
                bout[lax.rem(m, slots), r] = din[m, r] + by_wide.astype(BF16)
                b_send(m, c).start()

            return 0

        lax.fori_loop(0, chunks, piece, 0)

    def gradients(m):
        s = lax.rem(m, LAG + 1)
        at[...] = abuf[s].T
        dyt[...] = din[m].T
        for n in range(0, 2 * ff, TILE):
            w = min(TILE, 2 * ff - n)
            acc_gu[:, n:n + w] += dot(at[...], dgu[s, :, n:n + w]).astype(BF16).astype(F32)
        for n in range(0, ff, TILE):
            w = min(TILE, ff - n)
            acc_d[:, n:n + w] += dot(dyt[...], hid[s, :, n:n + w]).astype(BF16).astype(F32)

    warm = sum(jnp.where(me == n, w, 0) for n, w in enumerate(warms))
    start = jnp.where(me == 0, 0, -1)

    def tick(i, _):
        @pl.when((i >= 0) & (i < micro) & (me < last))
        def _():
            forward(i)

        @pl.when(i == start)
        def _():
            wdt[...] = wd[...].T
            for n in range(0, 2 * ff, TILE):
                w = min(TILE, 2 * ff - n)
                wgut[n:n + w] = wgu[:, n:n + w].T
            acc_gu[...] = jnp.zeros_like(acc_gu)
            acc_d[...] = jnp.zeros_like(acc_d)

        b = i - warm

        @pl.when((b >= 0) & (b < micro))
        def _():
            backward(b)

        @pl.when((b >= LAG) & (b < micro + LAG))
        def _():
            gradients(b - LAG)

        return 0

    lax.fori_loop(start, micro + warm + LAG, tick, 0)

    out_gu, out_d = dgu.at[0], wd
    stores = []
    out_gu[:, :ff] = acc_gu[:, :ff].astype(BF16)
    stores.append(pltpu.make_async_copy(out_gu.at[:, pl.ds(0, ff)], og_ref.at[0], osem.at[0]))
    stores[-1].start()
    out_gu[:, ff:] = acc_gu[:, ff:].astype(BF16)
    for n, (dst, src) in enumerate(up_parts()):
        stores.append(pltpu.make_async_copy(out_gu.at[:, pl.ds(*src)], ou_ref.at[0, :, pl.ds(*dst)], osem.at[1 + n]))
        stores[-1].start()
    out_d[...] = acc_d[...].astype(BF16).T
    stores.append(pltpu.make_async_copy(out_d, od_ref.at[0], osem.at[3]))
    stores[-1].start()

    def drain(send):
        def go(n, _):
            send(micro - slots + n // chunks, lax.rem(n, chunks)).wait_send()
            return 0

        lax.fori_loop(0, slots * chunks, go, 0)

    @pl.when(me < last)
    def _():
        drain(f_send)

    @pl.when(me > 0)
    def _():
        drain(b_send)

    for copy in stores:
        copy.wait()


def solution(mesh):
    stages = mesh.shape["pp"]

    def step(x, dy, wg, wu, wd):
        micro, tokens, d = x.shape
        ff = wg.shape[-1]
        cfg = (micro, tokens, d, ff, stages, WARM[:stages] if stages == len(WARM) else tuple(stages - 1 - n for n in range(stages)))
        hbm = pl.BlockSpec(memory_space=pl.ANY)
        keep = LAG + 1
        flops = 2 * micro * tokens * d * ff * 11
        return pl.pallas_call(
            functools.partial(kernel, cfg),
            out_shape=(
                jax.ShapeDtypeStruct((1, d, ff), BF16),
                jax.ShapeDtypeStruct((1, d, ff), BF16),
                jax.ShapeDtypeStruct((1, ff, d), BF16),
            ),
            in_specs=[hbm] * 5,
            out_specs=(hbm,) * 3,
            scratch_shapes=[
                pltpu.VMEM((micro, tokens, d), BF16),
                pltpu.VMEM((micro, tokens, d), BF16),
                pltpu.VMEM((d, 2 * ff), BF16),
                pltpu.VMEM((2 * ff, d), BF16),
                pltpu.VMEM((ff, d), BF16),
                pltpu.VMEM((d, ff), BF16),
                pltpu.VMEM((d, 2 * ff), F32),
                pltpu.VMEM((d, ff), F32),
                pltpu.VMEM((SLOTS, tokens, d), BF16),
                pltpu.VMEM((SLOTS, tokens, d), BF16),
                pltpu.VMEM((keep, tokens, 2 * ff), BF16),
                pltpu.VMEM((keep, tokens, ff), BF16),
                pltpu.VMEM((keep, tokens, d), BF16),
                pltpu.VMEM((d, tokens), BF16),
                pltpu.VMEM((d, tokens), BF16),
                pltpu.VMEM((tokens // CHUNKS, ff), BF16),
                pltpu.SemaphoreType.DMA((micro, CHUNKS)),
                pltpu.SemaphoreType.DMA((micro, CHUNKS)),
                pltpu.SemaphoreType.DMA((SLOTS, CHUNKS)),
                pltpu.SemaphoreType.DMA((SLOTS, CHUNKS)),
                pltpu.SemaphoreType.DMA((4,)),
                pltpu.SemaphoreType.DMA((4,)),
            ],
            compiler_params=pltpu.CompilerParams(collective_id=0, has_side_effects=True, vmem_limit_bytes=67_000_000),
            cost_estimate=pl.CostEstimate(flops=flops, bytes_accessed=40_000_000, transcendentals=0),
            name="pipeline",
        )(x, dy, wg, wu, wd)

    return jax.shard_map(
        step,
        mesh=mesh,
        in_specs=(P("rep", None, None),) * 2 + (P("pp", None, None),) * 3,
        out_specs=(P(("rep", "pp"), None, None),) * 3,
        check_vma=False,
    )
```

```python
import functools

import jax
import jax.numpy as jnp
from jax import lax
from jax.experimental import pallas as pl
from jax.experimental.pallas import tpu as pltpu
from jax.sharding import PartitionSpec as P

F32, BF16 = jnp.float32, jnp.bfloat16
CHUNKS, FINE = 2, 4
FIRST, FINAL = 1, 1
SLOTS = 2
ORDER = (
    "FTFFFFFFFFFFFFFBFBFWBBWBWWBBWBWBWBWBWBWBWBWWBBWWW",
    "TFFFFFFFFFFFFFBFBFWBFBWBWWBBWBWBWBWBWBWBWBWWBBWWW",
    "TFFFFFFBFFFFBFFWFBFBFBFBWBWBWBWBWBWBWBWBWWBBWWWWW",
    "TFFFFFBFFFFBFWFFBFBFBFBFBWBWBWBWBWBWBWBWWBBWWWWWW",
    "TFFFBFFFBFWFBFFBFBFBFBFBFBFBBWWBWBWBWWBBWWWWWWWWW",
    "TFFBFFFBFWBFFBFBFBFBFBFBFBFBFBWBWBWWBBWWWWWWWWWWW",
    "TFBFBFWFBFWBFBFBFBFBFBFBFBFBFBFBFBBWWWWWWWWWWWWWW",
    "TBBBWBBWBBWBBWBBWBBWBBBWWWWWWWWWW",
)
TILE = 256


def packed(order):
    codes = ["TFBW".index(step) for step in order]
    return [sum(code * 4**n for n, code in enumerate(codes[k:k + 15])) for k in range(0, len(codes), 15)]


def dot(a, b):
    return jnp.dot(a, b, preferred_element_type=F32)


def columns(ff):
    full, rest = divmod(ff, TILE)
    out = [(j * TILE, ff + rest + j * TILE, TILE) for j in range(full)]
    if rest:
        out.append((full * TILE, ff, rest))
    return out


def scale_of(wide):
    return lax.rsqrt(jnp.mean(wide * wide, -1, keepdims=True) + 1e-6)


def normed(h):
    wide = h.astype(F32)
    return (wide * scale_of(wide)).astype(BF16)


def kernel(cfg, x_ref, dy_ref, wg_ref, wu_ref, wd_ref, og_ref, ou_ref, od_ref, pq_hbm, hid_hbm, dgu_hbm, hin, din, wgu, wgut, wd, wdt, acc_gu, acc_d, hout, bout,
           at, dyt, hidf, fst, bst, gst, wgin, whin, fsem, bsem, fsend, bsend, fss, hss, bss, gss, ws, wsem, osem):
    micro, tokens, d, ff, stages, orders = cfg
    unit = tokens // FINE
    full, rest = divmod(ff, TILE)
    body = full * TILE
    me = lax.axis_index("pp")
    last = stages - 1

    def by_stage(table):
        return sum(jnp.where(me == n, w, 0) for n, w in enumerate(table))

    words = [packed(order) for order in orders]
    steps = by_stage([len(order) for order in orders])

    def code(k):
        word = sum(jnp.where(k // 15 == j, by_stage([w[j] if j < len(w) else 0 for w in words]), 0) for j in range(max(map(len, words))))
        return (word // sum(jnp.where(k % 15 == j, 4**j, 0) for j in range(15))) % 4

    def is_fine(m):
        return (m < FIRST) | (m >= micro - FINAL)

    def sized(m, go):
        @pl.when(is_fine(m))
        def _():
            go(unit, FINE)

        @pl.when(jnp.logical_not(is_fine(m)))
        def _():
            go(tokens // CHUNKS, CHUNKS)

    def up_parts():
        parts = [((0, body), (ff + rest, body))]
        if rest:
            parts.append(((body, rest), (ff, rest)))
        return parts

    def span(c, rows):
        return pl.ds(pl.multiple_of(c * rows, rows), rows)

    def first_of(c, rows):
        return c * (rows // unit)

    def h_in(m, c, rows):
        r = span(c, rows)
        return pltpu.make_async_copy(x_ref.at[m, r], hin.at[m, r], fsem.at[m, first_of(c, rows)])

    def d_in(m, c, rows):
        r = span(c, rows)
        return pltpu.make_async_copy(dy_ref.at[m, r], din.at[m, r], bsem.at[m, first_of(c, rows)])

    def f_send(m, c, rows):
        r, s = span(c, rows), lax.rem(m, SLOTS)
        return pltpu.make_async_remote_copy(
            src_ref=hout.at[s, r], dst_ref=hin.at[m, r], send_sem=fsend.at[s, first_of(c, rows)], recv_sem=fsem.at[m, first_of(c, rows)],
            device_id={"pp": me + 1})

    def b_send(m, c, rows):
        r, s = span(c, rows), lax.rem(m, SLOTS)
        return pltpu.make_async_remote_copy(
            src_ref=bout.at[s, r], dst_ref=din.at[m, r], send_sem=bsend.at[s, first_of(c, rows)], recv_sem=bsem.at[m, first_of(c, rows)],
            device_id={"pp": me - 1})

    def keep_pq(m, c, rows):
        p = lax.rem(c, 2)
        return pltpu.make_async_copy(fst.at[p, pl.ds(0, rows)], pq_hbm.at[m, span(c, rows)], fss.at[p])

    def keep_hid(m, c, rows):
        p = lax.rem(c, 2)
        return pltpu.make_async_copy(hidf.at[p, pl.ds(0, rows)], hid_hbm.at[m, span(c, rows)], hss.at[p])

    def keep_dgu(m, c, rows):
        p = lax.rem(c, 2)
        return pltpu.make_async_copy(gst.at[p, pl.ds(0, rows)], dgu_hbm.at[m, span(c, rows)], gss.at[p])

    def fetch(m, c, rows):
        p = lax.rem(c, 2)
        return pltpu.make_async_copy(pq_hbm.at[m, span(c, rows)], bst.at[p, pl.ds(0, rows)], bss.at[p])

    def fetch_w(m):
        p = lax.rem(m, 2)
        return [pltpu.make_async_copy(dgu_hbm.at[m], wgin.at[p], ws.at[p, 0]), pltpu.make_async_copy(hid_hbm.at[m], whin.at[p], ws.at[p, 1])]

    def pieces(n, go):
        def one(c, _):
            go(c)
            return 0

        lax.fori_loop(0, n, one, 0)

    def sent(send, m):
        sized(m, lambda rows, n: pieces(n, lambda c: send(m, c, rows).wait_send()))

    loads = [pltpu.make_async_copy(wg_ref.at[0], wgu.at[:, pl.ds(0, ff)], wsem.at[0])]
    for n, (src, dst) in enumerate(up_parts()):
        loads.append(pltpu.make_async_copy(wu_ref.at[0, :, pl.ds(*src)], wgu.at[:, pl.ds(*dst)], wsem.at[1 + n]))
    loads.append(pltpu.make_async_copy(wd_ref.at[0], wd, wsem.at[3]))

    @pl.when(me == 0)
    def _():
        sized(0, lambda rows, n: pieces(n, lambda c: h_in(0, c, rows).start()))

    for copy in loads:
        copy.start()

    @pl.when(me == 0)
    def _():
        def go(m, _):
            sized(m, lambda rows, n: pieces(n, lambda c: h_in(m, c, rows).start()))
            return 0

        lax.fori_loop(1, micro, go, 0)

    @pl.when(me == last)
    def _():
        def go(m, _):
            sized(m, lambda rows, n: pieces(n, lambda c: d_in(m, c, rows).start()))
            return 0

        lax.fori_loop(0, micro, go, 0)

    barrier = pltpu.get_barrier_semaphore()

    @pl.when(me > 0)
    def _():
        pl.semaphore_signal(barrier, inc=1, device_id={"pp": me - 1})

    @pl.when(me < last)
    def _():
        pl.semaphore_signal(barrier, inc=1, device_id={"pp": me + 1})

    @pl.when((me > 0) & (me < last))
    def _():
        pl.semaphore_wait(barrier, 2)

    @pl.when((me == 0) | (me == last))
    def _():
        pl.semaphore_wait(barrier, 1)

    for copy in loads:
        copy.wait()

    def pairs(a):
        for g0, u0, w in columns(ff):
            if w == TILE:
                g, u = dot(a, wgu[:, g0:g0 + w]), dot(a, wgu[:, u0:u0 + w])
            else:
                gu = dot(a, wgu[:, g0:g0 + 2 * w])
                g, u = gu[:, :w], gu[:, w:]
            yield g0, u0, w, g, u

    def units(a, to, p, rows):
        for g0, u0, w, g, u in pairs(a):
            sig = lax.logistic(g)
            silu = g * sig
            hidf[p, :rows, g0:g0 + w] = (silu * u).astype(BF16)
            to[p, :rows, g0:g0 + w] = u * (sig + silu * (1.0 - sig))
            to[p, :rows, u0:u0 + w] = silu

    def forward(m, settled, rows, n):
        def piece(c):
            r, p = span(c, rows), lax.rem(c, 2)
            h_in(m, c, rows).wait()

            @pl.when(c >= 2)
            def _():
                keep_pq(m, c - 2, rows).wait()
                keep_hid(m, c - 2, rows).wait()

            @pl.when((c < 2) & (settled < m))
            def _():
                sized(m - 1, lambda rows, n: [keep_pq(m - 1, n - 2 + c, rows).wait(), keep_hid(m - 1, n - 2 + c, rows).wait()])

            h = hin[m, r]
            units(normed(h), fst, p, rows)
            hout[lax.rem(m, SLOTS), r] = h + dot(hidf[p, :rows], wd[...]).astype(BF16)
            f_send(m, c, rows).start()
            keep_pq(m, c, rows).start()
            keep_hid(m, c, rows).start()

        pieces(n, piece)

    def settle_f(m):
        sized(m, lambda rows, n: [keep(m, n - k, rows).wait() for k in (2, 1) for keep in (keep_pq, keep_hid)])

    def settle_b(m):
        def go(rows, n):
            for k in (2, 1):
                keep_dgu(m, n - k, rows).wait()

            @pl.when(me == last)
            def _():
                for k in (2, 1):
                    keep_hid(m, n - k, rows).wait()

        sized(m, go)

    def backward(m, settled, more, rows, n):
        def piece(c):
            r, p = span(c, rows), lax.rem(c, 2)

            @pl.when(c >= 2)
            def _():
                keep_dgu(m, c - 2, rows).wait()

            @pl.when((c < 2) & (settled < m))
            def _():
                sized(m - 1, lambda rows, n: keep_dgu(m - 1, n - 2 + c, rows).wait())

            @pl.when(me == last)
            def _():
                h_in(m, c, rows).wait()

                @pl.when(c >= 2)
                def _():
                    keep_hid(m, c - 2, rows).wait()

                @pl.when((c < 2) & (settled < m))
                def _():
                    sized(m - 1, lambda rows, n: keep_hid(m - 1, n - 2 + c, rows).wait())

                units(normed(hin[m, r]), bst, p, rows)
                keep_hid(m, c, rows).start()

            @pl.when(me < last)
            def _():
                fetch(m, c, rows).wait()

            d_in(m, c, rows).wait()
            by_y = din[m, r]
            for g0, u0, w in columns(ff):
                by_z = dot(by_y, wdt[:, g0:g0 + w]).astype(BF16).astype(F32)
                gst[p, :rows, g0:g0 + w] = (by_z * bst[p, :rows, g0:g0 + w]).astype(BF16)
                gst[p, :rows, u0:u0 + w] = (by_z * bst[p, :rows, u0:u0 + w]).astype(BF16)
            by_a = dot(gst[p, :rows, :ff], wgut[:ff]).astype(BF16) + dot(gst[p, :rows, ff:], wgut[ff:]).astype(BF16)
            by_a = by_a.astype(F32)
            wide = hin[m, r].astype(F32)
            scale = scale_of(wide)
            by_scale = jnp.sum(by_a * wide, -1, keepdims=True)
            by_wide = by_a * scale - wide * (by_scale * scale * scale * scale * (1.0 / d))
            bout[lax.rem(m, SLOTS), r] = by_y + by_wide.astype(BF16)

            @pl.when(me > 0)
            def _():
                b_send(m, c, rows).start()

            keep_dgu(m, c, rows).start()

            @pl.when((me < last) & (c + 2 < n))
            def _():
                fetch(m, c + 2, rows).start()

            @pl.when(more & (c + 2 >= n))
            def _():
                sized(m + 1, lambda rows, _: fetch(m + 1, c + 2 - n, rows).start())

        pieces(n, piece)

    def gradients(m):
        p = lax.rem(m, 2)
        dyt[...] = din[m].T
        at[...] = normed(hin[m]).T
        for n in range(0, ff, TILE):
            w = min(TILE, ff - n)
            acc_d[:, n:n + w] += dot(dyt[...], whin[p, :, n:n + w]).astype(BF16).astype(F32)
        for n in range(0, 2 * ff, TILE):
            w = min(TILE, 2 * ff - n)
            acc_gu[:, n:n + w] += dot(at[...], wgin[p, :, n:n + w]).astype(BF16).astype(F32)

    def step(k, carry):
        now, nf, nb, nw, kf, kb, ab, aw = carry
        after = jnp.where(k + 1 < steps, code(k + 1), 0)
        is_f, is_b, is_w = (now == n for n in (1, 2, 3))

        w_next = jnp.where(is_w, jnp.where(aw > nw, nw + 1, nw), nw)
        ask_w = jnp.where(is_w & (aw <= nw), True, (after == 3) & (w_next < nb) & (aw <= w_next))
        b_next = nb
        ask_b = (me < last) & (ab <= nb) & (nb < nf) & (is_b | (after == 2))
        go_f = ((ask_b & (kf <= b_next)) | (is_b & (after == 2) & (me < last) & (nb + 1 < nf) & (kf <= nb + 1))) & (kf < nf)
        go_b = ask_w & (kb <= w_next) & (kb < nb)

        @pl.when(go_f)
        def _():
            settle_f(nf - 1)

        @pl.when(go_b)
        def _():
            settle_b(nb - 1)

        @pl.when(ask_b)
        def _():
            sized(b_next, lambda rows, n: [fetch(b_next, 0, rows).start(), fetch(b_next, 1, rows).start()])

        @pl.when(ask_w)
        def _():
            for copy in fetch_w(w_next):
                copy.start()

        kf, kb = jnp.where(go_f, nf, kf), jnp.where(go_b, nb, kb)
        ab, aw = jnp.where(ask_b, nb + 1, ab), jnp.where(ask_w, w_next + 1, aw)
        more = is_b & (after == 2) & (me < last) & (nb + 1 < nf)

        @pl.when(now == 0)
        def _():
            wdt[...] = wd[...].T
            for n in range(0, 2 * ff, TILE):
                w = min(TILE, 2 * ff - n)
                wgut[n:n + w] = wgu[:, n:n + w].T
            acc_gu[...] = jnp.zeros_like(acc_gu)
            acc_d[...] = jnp.zeros_like(acc_d)

        @pl.when(is_f)
        def _():
            @pl.when(nf >= SLOTS)
            def _():
                sent(f_send, nf - SLOTS)

            sized(nf, lambda rows, n: forward(nf, kf, rows, n))

        @pl.when(is_b)
        def _():
            @pl.when((nb >= SLOTS) & (me > 0))
            def _():
                sent(b_send, nb - SLOTS)

            sized(nb, lambda rows, n: backward(nb, kb, more, rows, n))

        @pl.when(is_w)
        def _():
            for copy in fetch_w(nw):
                copy.wait()
            gradients(nw)

        ab = jnp.where(more, nb + 2, ab)
        kf = jnp.where(is_f, nf, kf)
        kb = jnp.where(is_b, nb, kb)
        one = lambda on: jnp.where(on, 1, 0)
        return after, nf + one(is_f), nb + one(is_b), nw + one(is_w), kf, kb, ab, aw

    zero = jnp.int32(0)
    end = lax.fori_loop(0, steps, step, (code(zero),) + (zero,) * 7)

    @pl.when((me < last) & (end[4] < micro))
    def _():
        settle_f(micro - 1)

    @pl.when(end[5] < micro)
    def _():
        settle_b(micro - 1)

    out_gu, out_d = wgin.at[0], wd
    stores = []
    out_gu[:, :ff] = acc_gu[:, :ff].astype(BF16)
    stores.append(pltpu.make_async_copy(out_gu.at[:, pl.ds(0, ff)], og_ref.at[0], osem.at[0]))
    stores[-1].start()
    out_gu[:, ff:] = acc_gu[:, ff:].astype(BF16)
    for n, (dst, src) in enumerate(up_parts()):
        stores.append(pltpu.make_async_copy(out_gu.at[:, pl.ds(*src)], ou_ref.at[0, :, pl.ds(*dst)], osem.at[1 + n]))
        stores[-1].start()
    out_d[...] = acc_d[...].astype(BF16).T
    stores.append(pltpu.make_async_copy(out_d, od_ref.at[0], osem.at[3]))
    stores[-1].start()

    for m in range(micro - SLOTS, micro):
        @pl.when(me < last)
        def _():
            sent(f_send, m)

        @pl.when(me > 0)
        def _():
            sent(b_send, m)

    for copy in stores:
        copy.wait()


def solution(mesh):
    stages = mesh.shape["pp"]

    def step(x, dy, wg, wu, wd):
        micro, tokens, d = x.shape
        ff = wg.shape[-1]
        orders = ORDER
        if stages != len(ORDER) or micro != ORDER[0].count("F"):
            orders = ["T" + ("" if n == stages - 1 else "F" * micro) + "B" * micro + "W" * micro for n in range(stages)]
        cfg = (micro, tokens, d, ff, stages, orders)
        hbm = pl.BlockSpec(memory_space=pl.ANY)
        flops = 2 * micro * tokens * d * ff * 9
        return pl.pallas_call(
            functools.partial(kernel, cfg),
            out_shape=(
                jax.ShapeDtypeStruct((1, d, ff), BF16),
                jax.ShapeDtypeStruct((1, d, ff), BF16),
                jax.ShapeDtypeStruct((1, ff, d), BF16),
                jax.ShapeDtypeStruct((micro, tokens, 2 * ff), F32),
                jax.ShapeDtypeStruct((micro, tokens, ff), BF16),
                jax.ShapeDtypeStruct((micro, tokens, 2 * ff), BF16),
            ),
            in_specs=[hbm] * 5,
            out_specs=(hbm,) * 6,
            scratch_shapes=[
                pltpu.VMEM((micro, tokens, d), BF16),
                pltpu.VMEM((micro, tokens, d), BF16),
                pltpu.VMEM((d, 2 * ff), BF16),
                pltpu.VMEM((2 * ff, d), BF16),
                pltpu.VMEM((ff, d), BF16),
                pltpu.VMEM((d, ff), BF16),
                pltpu.VMEM((d, 2 * ff), F32),
                pltpu.VMEM((d, ff), F32),
                pltpu.VMEM((SLOTS, tokens, d), BF16),
                pltpu.VMEM((SLOTS, tokens, d), BF16),
                pltpu.VMEM((d, tokens), BF16),
                pltpu.VMEM((d, tokens), BF16),
                pltpu.VMEM((2, tokens // CHUNKS, ff), BF16),
                pltpu.VMEM((2, tokens // CHUNKS, 2 * ff), F32),
                pltpu.VMEM((2, tokens // CHUNKS, 2 * ff), F32),
                pltpu.VMEM((2, tokens // CHUNKS, 2 * ff), BF16),
                pltpu.VMEM((2, tokens, 2 * ff), BF16),
                pltpu.VMEM((2, tokens, ff), BF16),
                pltpu.SemaphoreType.DMA((micro, FINE)),
                pltpu.SemaphoreType.DMA((micro, FINE)),
                pltpu.SemaphoreType.DMA((SLOTS, FINE)),
                pltpu.SemaphoreType.DMA((SLOTS, FINE)),
                pltpu.SemaphoreType.DMA((2,)),
                pltpu.SemaphoreType.DMA((2,)),
                pltpu.SemaphoreType.DMA((2,)),
                pltpu.SemaphoreType.DMA((2,)),
                pltpu.SemaphoreType.DMA((2, 2)),
                pltpu.SemaphoreType.DMA((4,)),
                pltpu.SemaphoreType.DMA((4,)),
            ],
            compiler_params=pltpu.CompilerParams(collective_id=0, has_side_effects=True, vmem_limit_bytes=67_000_000),
            cost_estimate=pl.CostEstimate(flops=flops, bytes_accessed=40_000_000, transcendentals=0),
            name="pipeline",
        )(x, dy, wg, wu, wd)[:3]

    return jax.shard_map(
        step,
        mesh=mesh,
        in_specs=(P("rep", None, None),) * 2 + (P("pp", None, None),) * 3,
        out_specs=(P(("rep", "pp"), None, None),) * 3,
        check_vma=False,
    )
```

```python
import functools

import jax
import jax.numpy as jnp
from jax import lax
from jax.experimental import pallas as pl
from jax.experimental.pallas import tpu as pltpu
from jax.sharding import PartitionSpec as P

F32, BF16 = jnp.float32, jnp.bfloat16
CHUNKS, FINE = 2, 4
FIRST, FINAL = 1, 1
SLOTS = 2
ORDER = (
    "FTFFFFFFFFFFFFFBFFBWBWBWBWBWBWBWBWBWBWBWBWBWBWBWW",
    "TFFFFFFFFFFFFFBFMFBWBWBWBWBWBWBWBWBWBWBWBWBWBWWW",
    "TFFFFFFFFFFBFMMMMFBWBWBWBWBWBWBWBWBWBWBWWWWWW",
    "TFFFFFFFFFBFMMMMMFBWBWBWBWBWBWBWBWBWBWWWWWWW",
    "TFFFFFFBFMMMMMMMMFBWBWBWBWBWBWBWWWWWWWWWW",
    "TFFFFFBFMMMMMMMMMFBWBWBWBWBWBWWWWWWWWWWW",
    "TFFBFMMMMMMMMMMMMFBWBWBWWWWWWWWWWWWWW",
    "TBBBWBBWBBWBBWBBWBBWBBWBWWWWWWWWW",
)
TILE = 256


SPAN = 9


def packed(order):
    codes = ["TFBWM".index(step) for step in order]
    return [sum(code * 8**n for n, code in enumerate(codes[k:k + SPAN + 1])) for k in range(0, len(codes), SPAN)]


def dot(a, b):
    return jnp.dot(a, b, preferred_element_type=F32)


def columns(ff):
    full, rest = divmod(ff, TILE)
    out = [(j * TILE, ff + rest + j * TILE, TILE) for j in range(full)]
    if rest:
        out.append((full * TILE, ff, rest))
    return out


def scale_of(wide):
    return lax.rsqrt(jnp.mean(wide * wide, -1, keepdims=True) + 1e-6)


def normed(h):
    wide = h.astype(F32)
    return (wide * scale_of(wide)).astype(BF16)


def kernel(cfg, x_ref, dy_ref, wg_ref, wu_ref, wd_ref, og_ref, ou_ref, od_ref, pq_hbm, hid_hbm, dgu_hbm, hin, din, wgu, wgut, wd, wdt, acc_gu, acc_d, hout, bout,
           at, dyt, hidf, fst, bst, gst, wgin, whin, fsem, bsem, fsend, bsend, fss, hss, bss, gss, ws, wsem, osem):
    micro, tokens, d, ff, stages, orders = cfg
    unit = tokens // FINE
    full, rest = divmod(ff, TILE)
    body = full * TILE
    me = lax.axis_index("pp")
    last = stages - 1

    def by_stage(table):
        return sum(jnp.where(me == n, w, 0) for n, w in enumerate(table))

    words = [packed(order) for order in orders]
    steps = by_stage([len(order) for order in orders])

    def word(j):
        return sum(jnp.where(j == k, by_stage([w[k] if k < len(w) else 0 for w in words]), 0) for k in range(max(map(len, words))))

    def is_fine(m):
        return (m < FIRST) | (m >= micro - FINAL)

    def sized(m, go):
        @pl.when(is_fine(m))
        def _():
            go(unit, FINE)

        @pl.when(jnp.logical_not(is_fine(m)))
        def _():
            go(tokens // CHUNKS, CHUNKS)

    def up_parts():
        parts = [((0, body), (ff + rest, body))]
        if rest:
            parts.append(((body, rest), (ff, rest)))
        return parts

    def span(c, rows):
        return pl.ds(pl.multiple_of(c * rows, rows), rows)

    def first_of(c, rows):
        return c * (rows // unit)

    def h_in(m, c, rows):
        r = span(c, rows)
        return pltpu.make_async_copy(x_ref.at[m, r], hin.at[m, r], fsem.at[m, first_of(c, rows)])

    def d_in(m, c, rows):
        r = span(c, rows)
        return pltpu.make_async_copy(dy_ref.at[m, r], din.at[m, r], bsem.at[m, first_of(c, rows)])

    def f_send(m, c, rows):
        r, s = span(c, rows), lax.rem(m, SLOTS)
        return pltpu.make_async_remote_copy(
            src_ref=hout.at[s, r], dst_ref=hin.at[m, r], send_sem=fsend.at[s, first_of(c, rows)], recv_sem=fsem.at[m, first_of(c, rows)],
            device_id={"pp": me + 1})

    def b_send(m, c, rows):
        r, s = span(c, rows), lax.rem(m, SLOTS)
        return pltpu.make_async_remote_copy(
            src_ref=bout.at[s, r], dst_ref=din.at[m, r], send_sem=bsend.at[s, first_of(c, rows)], recv_sem=bsem.at[m, first_of(c, rows)],
            device_id={"pp": me - 1})

    def keep_pq(m, c, rows):
        p = lax.rem(c, 2)
        return pltpu.make_async_copy(fst.at[p, pl.ds(0, rows)], pq_hbm.at[m, span(c, rows)], fss.at[p])

    def keep_hid(m, c, rows):
        p = lax.rem(c, 2)
        return pltpu.make_async_copy(hidf.at[p, pl.ds(0, rows)], hid_hbm.at[m, span(c, rows)], hss.at[p])

    def keep_dgu(m, c, rows):
        p = lax.rem(c, 2)
        return pltpu.make_async_copy(gst.at[p, pl.ds(0, rows)], dgu_hbm.at[m, span(c, rows)], gss.at[p])

    def fetch(m, c, rows):
        p = lax.rem(c, 2)
        return pltpu.make_async_copy(pq_hbm.at[m, span(c, rows)], bst.at[p, pl.ds(0, rows)], bss.at[p])

    def fetch_w(m):
        p = lax.rem(m, 2)
        return [pltpu.make_async_copy(dgu_hbm.at[m], wgin.at[p], ws.at[p, 0]), pltpu.make_async_copy(hid_hbm.at[m], whin.at[p], ws.at[p, 1])]

    def pieces(n, go):
        def one(c, _):
            go(c)
            return 0

        lax.fori_loop(0, n, one, 0)

    def sent(send, m):
        sized(m, lambda rows, n: pieces(n, lambda c: send(m, c, rows).wait_send()))

    loads = [pltpu.make_async_copy(wg_ref.at[0], wgu.at[:, pl.ds(0, ff)], wsem.at[0])]
    for n, (src, dst) in enumerate(up_parts()):
        loads.append(pltpu.make_async_copy(wu_ref.at[0, :, pl.ds(*src)], wgu.at[:, pl.ds(*dst)], wsem.at[1 + n]))
    loads.append(pltpu.make_async_copy(wd_ref.at[0], wd, wsem.at[3]))

    @pl.when(me == 0)
    def _():
        sized(0, lambda rows, n: pieces(n, lambda c: h_in(0, c, rows).start()))

    for copy in loads:
        copy.start()

    @pl.when(me == 0)
    def _():
        def go(m, _):
            sized(m, lambda rows, n: pieces(n, lambda c: h_in(m, c, rows).start()))
            return 0

        lax.fori_loop(1, micro, go, 0)

    @pl.when(me == last)
    def _():
        def go(m, _):
            sized(m, lambda rows, n: pieces(n, lambda c: d_in(m, c, rows).start()))
            return 0

        lax.fori_loop(0, micro, go, 0)

    barrier = pltpu.get_barrier_semaphore()

    @pl.when(me > 0)
    def _():
        pl.semaphore_signal(barrier, inc=1, device_id={"pp": me - 1})

    @pl.when(me < last)
    def _():
        pl.semaphore_signal(barrier, inc=1, device_id={"pp": me + 1})

    @pl.when((me > 0) & (me < last))
    def _():
        pl.semaphore_wait(barrier, 2)

    @pl.when((me == 0) | (me == last))
    def _():
        pl.semaphore_wait(barrier, 1)

    for copy in loads:
        copy.wait()

    def pairs(a):
        for g0, u0, w in columns(ff):
            if w == TILE:
                g, u = dot(a, wgu[:, g0:g0 + w]), dot(a, wgu[:, u0:u0 + w])
            else:
                gu = dot(a, wgu[:, g0:g0 + 2 * w])
                g, u = gu[:, :w], gu[:, w:]
            yield g0, u0, w, g, u

    def units(a, to, p, rows):
        for g0, u0, w, g, u in pairs(a):
            sig = lax.logistic(g)
            silu = g * sig
            hidf[p, :rows, g0:g0 + w] = (silu * u).astype(BF16)
            to[p, :rows, g0:g0 + w] = u * (sig + silu * (1.0 - sig))
            to[p, :rows, u0:u0 + w] = silu

    def forward(m, settled, rows, n):
        def piece(c):
            r, p = span(c, rows), lax.rem(c, 2)
            h_in(m, c, rows).wait()

            @pl.when(c >= 2)
            def _():
                keep_pq(m, c - 2, rows).wait()
                keep_hid(m, c - 2, rows).wait()

            @pl.when((c < 2) & (settled < m))
            def _():
                sized(m - 1, lambda rows, n: [keep_pq(m - 1, n - 2 + c, rows).wait(), keep_hid(m - 1, n - 2 + c, rows).wait()])

            h = hin[m, r]
            units(normed(h), fst, p, rows)
            hout[lax.rem(m, SLOTS), r] = h + dot(hidf[p, :rows], wd[...]).astype(BF16)
            f_send(m, c, rows).start()
            keep_pq(m, c, rows).start()
            keep_hid(m, c, rows).start()

        return piece

    def settle_f(m):
        sized(m, lambda rows, n: [keep(m, n - k, rows).wait() for k in (2, 1) for keep in (keep_pq, keep_hid)])

    def settle_b(m):
        def go(rows, n):
            for k in (2, 1):
                keep_dgu(m, n - k, rows).wait()

            @pl.when(me == last)
            def _():
                for k in (2, 1):
                    keep_hid(m, n - k, rows).wait()

        sized(m, go)

    def backward(m, settled, more, rows, n):
        def piece(c):
            r, p = span(c, rows), lax.rem(c, 2)

            @pl.when(c >= 2)
            def _():
                keep_dgu(m, c - 2, rows).wait()

            @pl.when((c < 2) & (settled < m))
            def _():
                sized(m - 1, lambda rows, n: keep_dgu(m - 1, n - 2 + c, rows).wait())

            @pl.when(me == last)
            def _():
                h_in(m, c, rows).wait()

                @pl.when(c >= 2)
                def _():
                    keep_hid(m, c - 2, rows).wait()

                @pl.when((c < 2) & (settled < m))
                def _():
                    sized(m - 1, lambda rows, n: keep_hid(m - 1, n - 2 + c, rows).wait())

                units(normed(hin[m, r]), bst, p, rows)
                keep_hid(m, c, rows).start()

            @pl.when(me < last)
            def _():
                fetch(m, c, rows).wait()

            d_in(m, c, rows).wait()

            def units_back():
                by_y = din[m, r]
                for g0, u0, w in columns(ff):
                    by_z = dot(by_y, wdt[:, g0:g0 + w]).astype(BF16).astype(F32)
                    gst[p, :rows, g0:g0 + w] = (by_z * bst[p, :rows, g0:g0 + w]).astype(BF16)
                    gst[p, :rows, u0:u0 + w] = (by_z * bst[p, :rows, u0:u0 + w]).astype(BF16)
                return by_y

            @pl.when(me == 0)
            def _():
                units_back()

            @pl.when(me > 0)
            def _():
                by_y = units_back()
                by_a = dot(gst[p, :rows, :ff], wgut[:ff]).astype(BF16) + dot(gst[p, :rows, ff:], wgut[ff:]).astype(BF16)
                by_a = by_a.astype(F32)
                wide = hin[m, r].astype(F32)
                scale = scale_of(wide)
                by_scale = jnp.sum(by_a * wide, -1, keepdims=True)
                by_wide = by_a * scale - wide * (by_scale * scale * scale * scale * (1.0 / d))
                bout[lax.rem(m, SLOTS), r] = by_y + by_wide.astype(BF16)
                b_send(m, c, rows).start()

            keep_dgu(m, c, rows).start()

            @pl.when((me < last) & (c + 2 < n))
            def _():
                fetch(m, c + 2, rows).start()

            @pl.when(more & (c + 2 >= n))
            def _():
                sized(m + 1, lambda rows, _: fetch(m + 1, c + 2 - n, rows).start())

        return piece

    def transposed(m):
        dyt[...] = din[m].T
        at[...] = normed(hin[m]).T

    def gradients(m):
        p = lax.rem(m, 2)
        transposed(m)
        for n in range(0, ff, TILE):
            w = min(TILE, ff - n)
            acc_d[:, n:n + w] += dot(dyt[...], whin[p, :, n:n + w]).astype(BF16).astype(F32)
        for n in range(0, 2 * ff, TILE):
            w = min(TILE, 2 * ff - n)
            acc_gu[:, n:n + w] += dot(at[...], wgin[p, :, n:n + w]).astype(BF16).astype(F32)

    final = (micro - 1) % 2
    out_gu, out_d = wgin.at[1 - final], wd
    stores = [pltpu.make_async_copy(out_d, od_ref.at[0], osem.at[0]), pltpu.make_async_copy(out_gu.at[:, pl.ds(0, ff)], og_ref.at[0], osem.at[1])]
    for n, (dst, src) in enumerate(up_parts()):
        stores.append(pltpu.make_async_copy(out_gu.at[:, pl.ds(*src)], ou_ref.at[0, :, pl.ds(*dst)], osem.at[2 + n]))

    def gradients_last():
        transposed(micro - 1)
        for n in range(0, ff, TILE):
            w = min(TILE, ff - n)
            total = acc_d[:, n:n + w] + dot(dyt[...], whin[final, :, n:n + w]).astype(BF16).astype(F32)
            out_d[n:n + w] = total.astype(BF16).T
        stores[0].start()
        for n in range(0, 2 * ff, TILE):
            w = min(TILE, 2 * ff - n)
            total = acc_gu[:, n:n + w] + dot(at[...], wgin[final, :, n:n + w]).astype(BF16).astype(F32)
            out_gu[:, n:n + w] = total.astype(BF16)
            if n < ff <= n + w:
                stores[1].start()
        for copy in stores[2:]:
            copy.start()

    def step(k, carry):
        rest, nf, nb, nw, kf, kb, ab, aw = carry
        now, rest = lax.rem(rest, 8), lax.div(rest, 8)
        after = lax.rem(rest, 8)
        after_b = (after == 2) | (after == 4)
        is_f, is_b, is_w = (now == 1) | (now == 4), (now == 2) | (now == 4), now == 3

        w_next = jnp.where(is_w, jnp.where(aw > nw, nw + 1, nw), nw)
        ask_w = jnp.where(is_w & (aw <= nw), True, (after == 3) & (w_next < nb) & (aw <= w_next))
        b_next = nb
        ask_b = (me < last) & (ab <= nb) & (nb < nf) & (is_b | after_b)
        go_f = ((ask_b & (kf <= b_next)) | (is_b & after_b & (me < last) & (nb + 1 < nf) & (kf <= nb + 1))) & (kf < nf)
        go_b = ask_w & (kb <= w_next) & (kb < nb)

        @pl.when(go_f)
        def _():
            settle_f(nf - 1)

        @pl.when(go_b)
        def _():
            settle_b(nb - 1)

        @pl.when(ask_b)
        def _():
            sized(b_next, lambda rows, n: [fetch(b_next, 0, rows).start(), fetch(b_next, 1, rows).start()])

        @pl.when(ask_w)
        def _():
            for copy in fetch_w(w_next):
                copy.start()

        kf, kb = jnp.where(go_f, nf, kf), jnp.where(go_b, nb, kb)
        ab, aw = jnp.where(ask_b, nb + 1, ab), jnp.where(ask_w, w_next + 1, aw)
        more = is_b & after_b & (me < last) & (nb + 1 < nf)

        @pl.when(now == 0)
        def _():
            wdt[...] = wd[...].T
            for n in range(0, 2 * ff, TILE):
                w = min(TILE, 2 * ff - n)
                wgut[n:n + w] = wgu[:, n:n + w].T
            acc_gu[...] = jnp.zeros_like(acc_gu)
            acc_d[...] = jnp.zeros_like(acc_d)

        @pl.when(is_f & (nf >= SLOTS))
        def _():
            sent(f_send, nf - SLOTS)

        @pl.when(is_b & (nb >= SLOTS) & (me > 0))
        def _():
            sent(b_send, nb - SLOTS)

        def work(rows, n):
            ahead, back = forward(nf, kf, rows, n), backward(nb, kb, more, rows, n)

            def piece(c):
                @pl.when(is_f)
                def _():
                    ahead(c)

                @pl.when(is_b)
                def _():
                    back(c)

            pieces(n, piece)

        @pl.when(is_f | is_b)
        def _():
            sized(jnp.where(is_f, nf, nb), work)

        @pl.when(is_w)
        def _():
            for copy in fetch_w(nw):
                copy.wait()

            @pl.when(nw < micro - 1)
            def _():
                gradients(nw)

            @pl.when(nw == micro - 1)
            def _():
                gradients_last()

        ab = jnp.where(more, nb + 2, ab)
        kf = jnp.where(is_f, nf, kf)
        kb = jnp.where(is_b, nb, kb)
        one = lambda on: jnp.where(on, 1, 0)
        return rest, nf + one(is_f), nb + one(is_b), nw + one(is_w), kf, kb, ab, aw

    zero = jnp.int32(0)

    def steps_of(j, carry):
        return lax.fori_loop(0, jnp.minimum(SPAN, steps - SPAN * j), step, (word(j),) + carry)[1:]

    end = (zero,) + lax.fori_loop(0, (steps + SPAN - 1) // SPAN, steps_of, (zero,) * 7)

    @pl.when((me < last) & (end[4] < micro))
    def _():
        settle_f(micro - 1)

    @pl.when(end[5] < micro)
    def _():
        settle_b(micro - 1)

    for m in range(micro - SLOTS, micro):
        @pl.when(me < last)
        def _():
            sent(f_send, m)

        @pl.when(me > 0)
        def _():
            sent(b_send, m)

    for copy in stores:
        copy.wait()


PARTS = 4


def hand_on(*refs):
    ins, outs, held, in_sem, out_sem = refs[:3], refs[3:6], refs[6:9], refs[9], refs[10]
    moves = []
    for n in range(3):
        rows = ins[n].shape[1] // PARTS
        for k in range(PARTS):
            r = pl.ds(k * rows, rows)
            moves.append((pltpu.make_async_copy(ins[n].at[:, r], held[n].at[:, r], in_sem.at[n, k]),
                          pltpu.make_async_copy(held[n].at[:, r], outs[n].at[:, r], out_sem.at[n, k])))
    for take, _ in moves:
        take.start()
    for take, put in moves:
        take.wait()
        put.start()
    for _, put in moves:
        put.wait()


def solution(mesh):
    stages = mesh.shape["pp"]

    def step(x, dy, wg, wu, wd):
        micro, tokens, d = x.shape
        ff = wg.shape[-1]
        orders = ORDER
        if stages != len(ORDER) or micro != ORDER[0].count("F") + ORDER[0].count("M"):
            orders = ["T" + ("" if n == stages - 1 else "F" * micro) + "B" * micro + "W" * micro for n in range(stages)]
        cfg = (micro, tokens, d, ff, stages, orders)
        hbm = pl.BlockSpec(memory_space=pl.ANY)
        flops = 2 * micro * tokens * d * ff * 9
        grads = pl.pallas_call(
            functools.partial(kernel, cfg),
            out_shape=(
                jax.ShapeDtypeStruct((1, d, ff), BF16),
                jax.ShapeDtypeStruct((1, d, ff), BF16),
                jax.ShapeDtypeStruct((1, ff, d), BF16),
                jax.ShapeDtypeStruct((micro, tokens, 2 * ff), F32),
                jax.ShapeDtypeStruct((micro, tokens, ff), BF16),
                jax.ShapeDtypeStruct((micro, tokens, 2 * ff), BF16),
            ),
            in_specs=[hbm] * 5,
            out_specs=(hbm,) * 6,
            scratch_shapes=[
                pltpu.VMEM((micro, tokens, d), BF16),
                pltpu.VMEM((micro, tokens, d), BF16),
                pltpu.VMEM((d, 2 * ff), BF16),
                pltpu.VMEM((2 * ff, d), BF16),
                pltpu.VMEM((ff, d), BF16),
                pltpu.VMEM((d, ff), BF16),
                pltpu.VMEM((d, 2 * ff), F32),
                pltpu.VMEM((d, ff), F32),
                pltpu.VMEM((SLOTS, tokens, d), BF16),
                pltpu.VMEM((SLOTS, tokens, d), BF16),
                pltpu.VMEM((d, tokens), BF16),
                pltpu.VMEM((d, tokens), BF16),
                pltpu.VMEM((2, tokens // CHUNKS, ff), BF16),
                pltpu.VMEM((2, tokens // CHUNKS, 2 * ff), F32),
                pltpu.VMEM((2, tokens // CHUNKS, 2 * ff), F32),
                pltpu.VMEM((2, tokens // CHUNKS, 2 * ff), BF16),
                pltpu.VMEM((2, tokens, 2 * ff), BF16),
                pltpu.VMEM((2, tokens, ff), BF16),
                pltpu.SemaphoreType.DMA((micro, FINE)),
                pltpu.SemaphoreType.DMA((micro, FINE)),
                pltpu.SemaphoreType.DMA((SLOTS, FINE)),
                pltpu.SemaphoreType.DMA((SLOTS, FINE)),
                pltpu.SemaphoreType.DMA((2,)),
                pltpu.SemaphoreType.DMA((2,)),
                pltpu.SemaphoreType.DMA((2,)),
                pltpu.SemaphoreType.DMA((2,)),
                pltpu.SemaphoreType.DMA((2, 2)),
                pltpu.SemaphoreType.DMA((4,)),
                pltpu.SemaphoreType.DMA((4,)),
            ],
            compiler_params=pltpu.CompilerParams(collective_id=0, has_side_effects=True, vmem_limit_bytes=67_000_000),
            cost_estimate=pl.CostEstimate(flops=flops, bytes_accessed=40_000_000, transcendentals=0),
            name="pipeline",
        )(x, dy, wg, wu, wd)[:3]
        return pl.pallas_call(
            hand_on,
            out_shape=tuple(jax.ShapeDtypeStruct(g.shape, g.dtype) for g in grads),
            in_specs=[hbm] * 3,
            out_specs=(hbm,) * 3,
            scratch_shapes=[pltpu.VMEM(g.shape, g.dtype) for g in grads] + [pltpu.SemaphoreType.DMA((3, PARTS))] * 2,
            compiler_params=pltpu.CompilerParams(vmem_limit_bytes=60_000_000),
            name="hand_on",
        )(*grads)

    return jax.shard_map(
        step,
        mesh=mesh,
        in_specs=(P("rep", None, None),) * 2 + (P("pp", None, None),) * 3,
        out_specs=(P(("rep", "pp"), None, None),) * 3,
        check_vma=False,
    )
```
